32 devices in a mesh: dom: 8 (over y, x, core), grp: 4 (over z).
Axes of the slice: x: 2, y: 2, z: 4, core: 2. Of those that a mesh axis runs over, the one named last changes fastest.
Arguments:
- solved: bfloat16 [8, 4096, 512], P('dom', 'grp'), may hold values from -6 to 6
- e_blocks: bfloat16 [8, 6, 4096, 1024], P('dom', None, 'grp'), may hold values from -0.125 to 0.125
- block_mask: int32 [8, 6, 4], P('dom', None, 'grp'), may hold values 0 or 1
- owner: int32 [8, 6, 1], P('dom'), may hold values from 0 to 7; in each aligned block of 6 rows (0 to 5, 6 to 11, ..., all dimensions but the last counted through in order) at most 2 rows name the same one
- local_id: int32 [8, 6], P('dom'), may hold values from 0 to 3
Outputs:
- schur: bfloat16 [32, 1024, 512], P('dom', 'grp')
The draws below stay inside these ranges and needn't reach their ends.
Inputs may be any that keep to these rules, and one draw needn't show every extreme that they name: Among the 6 slots of one subdomain at most 2 have the same owner, and in some subdomain exactly 2 do.
All inputs are finite; a program needn't handle non-finite values. No bound on the sum of `block_mask` on one device may be relied on, other than what follows from the above.
Results may differ from the reference program's by a relative error of at most 0.015.
Values may be sent and summed in bfloat16 or wider, within the bound.
A program may use at most 128 MiB of HBM per device.

```python
import math
import jax
import jax.numpy as jnp
import numpy as np
from jax import lax

BLK = 1024
COLS = 512
SLOTS = 6
RBLK_DEV = 1
OWN = 4
CAP = 2
NRB = 4
ROWS = 4096
N_DOM = 8
N_GRP = 4


def place_ends(result, key, least, high):
    longest = result.shape.index(max(result.shape))
    spots = []
    for shift in (0, 1):
        where = [jax.random.randint(jax.random.fold_in(key, axis), (), 0, length) for axis, length in enumerate(result.shape)]
        where[longest] = (where[longest] + shift) % result.shape[longest]
        spots.append(tuple(where))
    return result.at[spots[0]].set(least).at[spots[1]].set(high)


def strengthened(values, stream_key, source, target, shards_of, factor):
    def block_of(dim):
        return (jnp.arange(values.shape[dim]) // (values.shape[dim] // shards_of)).reshape((-1,) + (1,) * (values.ndim - 1 - dim))

    first = jax.random.permutation(stream_key, shards_of)[block_of(target)]
    far = (block_of(target) + shards_of // 2) % shards_of
    return jnp.where((block_of(source) == first) | (block_of(source) == far), factor * values, values)


def block_scale(rng, shape, split, low, top_value):
    factor_of = 1.0
    for axis_at, shards_of in split:
        heights = jax.random.uniform(jax.random.fold_in(jax.random.fold_in(rng, 6), axis_at), (shards_of,), jnp.float32, low / len(split), top_value / len(split))
        factor_of = factor_of * jnp.repeat(jnp.exp(heights), shape[axis_at] // shards_of).reshape((-1,) + (1,) * (len(shape) - 1 - axis_at))
    return factor_of


def routed_block(key, own, number, rows, amount, top, bound, slope):
    ranking = jax.random.permutation(key, amount)
    heavy_load, ordinary = portions_of(amount, rows * top, bound, slope, True), portions_of(amount, rows * top, bound, slope, False)
    places = jnp.arange(amount)

    def named(sizes, turn):
        used = int((sizes > 0).sum())
        fixed = max(1, used // 4)
        shifted = fixed + (places - fixed + turn * (used - fixed)) % max(1, amount - fixed)
        return jnp.zeros((amount,), jnp.int32).at[ranking[jnp.where(places < fixed, places, shifted)]].set(jnp.asarray(sizes, jnp.int32))

    sizes = jnp.where(number % 4 == 0, named(heavy_load, number // 4), named(ordinary, number - number // 4 - 1))
    mixed = jax.random.permutation(jax.random.fold_in(own, 3), amount)
    source_of, sink = mixed[0:amount // 2 * 2:2], mixed[1:amount // 2 * 2:2]
    margin = jnp.minimum(sizes[source_of] - 1, bound - sizes[sink]) // 2
    margin = jnp.where((source_of == ranking[0]) | (sink == ranking[0]) | (sizes[sink] == 0), 0, jnp.maximum(margin, 0))
    shifted = jax.random.randint(jax.random.fold_in(own, 4), (amount // 2,), 0, 1 << 20) % (margin + 1)
    sizes = sizes.at[source_of].add(-shifted).at[sink].add(shifted)
    labels = jnp.searchsorted(jnp.cumsum(sizes), jnp.arange(rows * top), side="right").astype(jnp.int32)
    table = labels.reshape(top, rows).T
    table = table[jax.random.permutation(jax.random.fold_in(own, 1), rows)]
    turn = jax.random.randint(jax.random.fold_in(own, 2), (rows, 1), 0, top)
    return jnp.take_along_axis(table, (jnp.arange(top)[None, :] + turn) % top, axis=1)


def portions_of(count, total, limit, lean, full):
    weights = [(1 << 20) // math.isqrt(rank ** lean) + 1 for rank in range(1, count + 1)]
    largest = limit if full else min(limit, max(-(-total // count), total * weights[0] // sum(weights)))
    least = 1 if total - largest >= count - 1 else 0
    holding, spare = [largest] + [least] * (count - 1), total - largest - least * (count - 1)
    while spare > 0:
        free = [i for i in range(1, count) if holding[i] < largest] or [i for i in range(1, count) if holding[i] < limit]
        mass, left = sum([weights[i] for i in free]), spare
        for i in free:
            extra = min(limit - holding[i], max(1, left * weights[i] // mass), spare)
            holding[i] = holding[i] + extra
            spare = spare - extra
    return np.array(holding)


def noise(own_key, shape, scale, limit, cuts=(), kind=jnp.bfloat16):
    result = scale * jax.random.normal(own_key, shape, jnp.float32)
    if cuts:
        result = result * block_scale(own_key, shape, cuts, -0.22, 0.18)
    return jnp.clip(result, -limit, limit).astype(kind)


def noise_with(stream_key, extent, width, most, cuts, heavy, kind=jnp.bfloat16):
    entries = width * jax.random.normal(stream_key, extent, jnp.float32)
    if cuts:
        entries = entries * block_scale(stream_key, extent, cuts, -0.22, 0.18)
    return jnp.clip(strengthened(entries, jax.random.fold_in(stream_key, 3), *heavy), -most, most).astype(kind)


def setup_inputs(seed: int = 0) -> dict:
    keys = jax.random.split(jax.random.key(seed), 6)
    solved = noise(keys[0], (N_DOM, ROWS, COLS), 1.0, 6.0, ((0, 8), (1, 4)))
    e_blocks = noise_with(keys[1], (N_DOM, SLOTS, ROWS, BLK), ROWS ** -0.5, 0.125, ((0, 8), (2, 4)), (2, 3, 4, 2.0))
    block_mask = place_ends((jax.random.randint(keys[2], (N_DOM, SLOTS, NRB), 0, 4) < 3).astype(jnp.int32), jax.random.fold_in(keys[2], 1), 0, 1)
    owner_keys = jax.random.split(jax.random.fold_in(keys[3], 1), N_DOM * SLOTS // SLOTS)
    owner_turns = jax.random.permutation(jax.random.fold_in(keys[3], 3), N_DOM * SLOTS // SLOTS)
    owner = jax.vmap(lambda own, number: routed_block(jax.random.fold_in(keys[3], 2), own, number, SLOTS, N_DOM, 1, CAP, 2))(owner_keys, owner_turns).reshape((N_DOM, SLOTS, 1))
    local_id = place_ends(jax.random.randint(keys[4], (N_DOM, SLOTS), 0, OWN), jax.random.fold_in(keys[4], 1), 0, OWN - 1).astype(jnp.int32)
    return {"solved": solved, "e_blocks": e_blocks, "block_mask": block_mask, "owner": owner, "local_id": local_id}


def one_domain(inputs):
    solved_part, coupling, present = inputs
    solved4 = solved_part.reshape(NRB, BLK, COLS).astype(jnp.float32)

    def one_slot(pair):
        slot_coupling, slot_present = pair
        coupling4 = slot_coupling.reshape(NRB, BLK, BLK).astype(jnp.float32)
        product = jnp.einsum("bjk,bjc->bkc", coupling4, solved4)
        weighted = product * slot_present.astype(jnp.float32)[:, None, None]
        partial_value = jnp.sum(weighted.reshape(N_GRP, RBLK_DEV, BLK, COLS), axis=1).astype(jnp.bfloat16)
        return jnp.sum(partial_value.astype(jnp.float32), axis=0).astype(jnp.bfloat16)

    return lax.map(one_slot, (coupling, present))


def reference(solved, e_blocks, block_mask, owner, local_id):
    contribution = lax.map(one_domain, (solved, e_blocks, block_mask))
    target = (owner[:, :, 0] * OWN + local_id).reshape(N_DOM * SLOTS).astype(jnp.int32)
    slots_all = jnp.arange(N_DOM * OWN, dtype=jnp.int32)
    select = (target[:, None] == slots_all[None, :]).astype(jnp.float32)
    flat = contribution.reshape(N_DOM * SLOTS, BLK, COLS).astype(jnp.float32)
    summed = jnp.einsum("nt,nkc->tkc", select, flat)
    return summed.astype(jnp.bfloat16)
```

```python
import functools

import jax
import jax.numpy as jnp
from jax import lax
from jax.experimental import pallas as pl
from jax.experimental.pallas import tpu as pltpu
from jax.sharding import PartitionSpec as P

OWN = 4
CAP = 2
LANES = 128


def kernel(
    n, n_dom, mask_ref, owner_ref, local_ref, solved_ref, e_ref, out_ref,
    factor_t, coupling, own, from_left, from_right, fin, outbox, inbox, label_out, label_in, total,
    e_sem, right_send, right_recv, left_send, left_recv, dom_send, dom_recv, label_send, label_recv,
):
    g = lax.axis_index("grp")
    me = lax.axis_index("dom")
    pieces, _, slots, width, rows = own.shape
    cols = factor_t.shape[0]

    fetches = [pltpu.make_async_copy(e_ref.at[s], coupling.at[s], e_sem.at[s]) for s in range(slots)]
    for fetch in fetches:
        fetch.start()

    barrier = pltpu.get_barrier_semaphore()

    @pl.when(g > 0)
    def _():
        pl.semaphore_signal(barrier, inc=1, device_id={"grp": g - 1})

    @pl.when(g < n - 1)
    def _():
        pl.semaphore_signal(barrier, inc=1, device_id={"grp": g + 1})

    def greet(off, carry):
        pl.semaphore_signal(barrier, inc=1, device_id={"dom": lax.rem(me + off, n_dom)})
        return carry

    lax.fori_loop(1, n_dom, greet, 0)

    for p in range(pieces):
        factor_t[p * width:(p + 1) * width, :] = solved_ref[:, p * width:(p + 1) * width].T

    def multiply(s, carry):
        pltpu.make_async_copy(e_ref.at[s], coupling.at[s], e_sem.at[s]).wait()
        present = mask_ref[s].astype(jnp.float32)
        for ch in range(n):
            product = jnp.dot(
                factor_t[...], coupling[s, :, ch * rows:(ch + 1) * rows], preferred_element_type=jnp.float32
            )
            own[:, ch, s] = (product * present).astype(jnp.bfloat16).reshape(pieces, width, rows)
        return carry

    lax.fori_loop(0, slots, multiply, 0)

    def place(d, j):
        index, label = jnp.int32(0), jnp.int32(0)
        for s in range(slots):
            position = jnp.int32(0)
            for t in range(s):
                position = position + jnp.where(owner_ref[t] == owner_ref[s], 1, 0)
            hit = jnp.where((owner_ref[s] == d) & (position == j), 1, 0)
            index = index + hit * s
            label = label + hit * (local_ref[s] + 1)
        return index, label

    def label_copy(d, source):
        return pltpu.make_async_remote_copy(
            src_ref=label_out.at[d], dst_ref=label_in.at[source],
            send_sem=label_send.at[d], recv_sem=label_recv.at[source], device_id={"dom": d},
        )

    def dom_copy(p, d, source):
        return pltpu.make_async_remote_copy(
            src_ref=outbox.at[p, d], dst_ref=inbox.at[p, source],
            send_sem=dom_send.at[p, d], recv_sem=dom_recv.at[p, source], device_id={"dom": d},
        )

    def right_copy(p, ch, source):
        return pltpu.make_async_remote_copy(
            src_ref=source.at[p, ch], dst_ref=from_left.at[p, ch],
            send_sem=right_send.at[p, ch], recv_sem=right_recv.at[p, ch], device_id={"grp": g + 1},
        )

    def left_copy(p, ch, source):
        return pltpu.make_async_remote_copy(
            src_ref=source.at[p, ch], dst_ref=from_right.at[p, ch],
            send_sem=left_send.at[p, ch], recv_sem=left_recv.at[p, ch], device_id={"grp": g - 1},
        )

    greeted = n_dom - 1 + jnp.where(g > 0, 1, 0) + jnp.where(g < n - 1, 1, 0)
    pl.semaphore_wait(barrier, greeted)

    def send_labels(off, carry):
        d = lax.rem(me + off, n_dom)
        for j in range(CAP):
            _, label = place(d, j)
            label_out[d, j] = jnp.full(label_out.shape[2:], label.astype(jnp.float32), jnp.float32)
        label_copy(d, me).start()
        return carry

    def add_to(buffer, p, ch):
        def one(s, carry):
            buffer[p, ch, s] = (
                buffer[p, ch, s].astype(jnp.float32) + own[p, ch, s].astype(jnp.float32)
            ).astype(jnp.bfloat16)
            return carry

        lax.fori_loop(0, slots, one, 0)

    def forward(p):
        def one(i, carry):
            to_right = n - 1 - i

            @pl.when((to_right > g) & (g == 0))
            def _():
                right_copy(p, to_right, own).start()

            @pl.when((i < g) & (g == n - 1))
            def _():
                left_copy(p, i, own).start()

            @pl.when((to_right > g) & (g > 0))
            def _():
                right_copy(p, to_right, from_left).wait_recv()
                add_to(from_left, p, to_right)
                right_copy(p, to_right, from_left).start()

            @pl.when((i < g) & (g < n - 1))
            def _():
                left_copy(p, i, from_right).wait_recv()
                add_to(from_right, p, i)
                left_copy(p, i, from_right).start()

            return carry

        lax.fori_loop(0, n - 1, one, 0)

    def finish(p):
        @pl.when(g > 0)
        def _():
            right_copy(p, g, from_left).wait_recv()
            add_to(from_left, p, g)

        @pl.when(g == 0)
        def _():
            left_copy(p, g, from_right).wait_recv()
            add_to(from_right, p, g)

            def one(s, carry):
                fin[s] = from_right[p, g, s]
                return carry

            lax.fori_loop(0, slots, one, 0)

        @pl.when(g == n - 1)
        def _():
            def one(s, carry):
                fin[s] = from_left[p, g, s]
                return carry

            lax.fori_loop(0, slots, one, 0)

        @pl.when((g > 0) & (g < n - 1))
        def _():
            left_copy(p, g, from_right).wait_recv()

            def one(s, carry):
                fin[s] = (
                    from_left[p, g, s].astype(jnp.float32) + from_right[p, g, s].astype(jnp.float32)
                ).astype(jnp.bfloat16)
                return carry

            lax.fori_loop(0, slots, one, 0)

        def one_domain(off, carry):
            d = lax.rem(me + off, n_dom)
            for j in range(CAP):
                index, _ = place(d, j)
                outbox[p, d, j] = fin[index]
            dom_copy(p, d, me).start()
            return carry

        lax.fori_loop(1, n_dom, one_domain, 0)
        for j in range(CAP):
            index, _ = place(me, j)
            inbox[p, me, j] = fin[index]

    tile = 32

    def merge(p):
        def arrive(off, carry):
            source = lax.rem(me + off, n_dom)
            dom_copy(p, source, source).wait_recv()
            return carry

        lax.fori_loop(1, n_dom, arrive, 0)

        def one(t, carry):
            at = pl.ds(pl.multiple_of(t * tile, tile), tile)
            sums = [jnp.zeros((tile, rows), jnp.float32) for _ in range(OWN)]
            for source in range(n_dom):
                for j in range(CAP):
                    block = inbox[p, source, j, at, :].astype(jnp.float32)
                    label = label_in[source, j, 0:1, :]
                    for o in range(OWN):
                        sums[o] = sums[o] + block * jnp.where(label == o + 1, 1.0, 0.0)
            for o in range(OWN):
                total[o, at, :] = sums[o]
            return carry

        lax.fori_loop(0, width // tile, one, 0)
        for o in range(OWN):
            out_ref[o, :, p * width:(p + 1) * width] = total[o].T.astype(jnp.bfloat16)

    forward(0)
    lax.fori_loop(1, n_dom, send_labels, 0)
    for j in range(CAP):
        _, label = place(me, j)
        label_in[me, j] = jnp.full(label_out.shape[2:], label.astype(jnp.float32), jnp.float32)
    for p in range(pieces):
        if p + 1 < pieces:
            forward(p + 1)
        finish(p)
        if p == 0:
            def labelled(off, carry):
                source = lax.rem(me + off, n_dom)
                label_copy(source, source).wait_recv()
                return carry

            lax.fori_loop(1, n_dom, labelled, 0)
        else:
            merge(p - 1)
    merge(pieces - 1)

    def drain_dom(off, carry):
        d = lax.rem(me + off, n_dom)
        label_copy(d, me).wait_send()
        for p in range(pieces):
            dom_copy(p, d, me).wait_send()
        return carry

    lax.fori_loop(1, n_dom, drain_dom, 0)

    def drain(ch, carry):
        for p in range(pieces):
            @pl.when(ch > g)
            def _():
                right_copy(p, ch, from_left).wait_send()

            @pl.when(ch < g)
            def _():
                left_copy(p, ch, from_right).wait_send()

        return carry

    lax.fori_loop(0, n, drain, 0)


def on_device(solved, e_blocks, block_mask, owner, local_id):
    n, n_dom = lax.axis_size("grp"), lax.axis_size("dom")
    _, depth, cols = solved.shape
    slots, blk = e_blocks.shape[1], e_blocks.shape[3]
    rows, width = blk // n, LANES
    pieces = cols // width
    bf16, f32 = jnp.bfloat16, jnp.float32
    smem = pl.BlockSpec(memory_space=pltpu.SMEM)
    dma = pltpu.SemaphoreType.DMA
    return pl.pallas_call(
        functools.partial(kernel, n, n_dom),
        out_shape=jax.ShapeDtypeStruct((OWN, rows, cols), bf16),
        in_specs=[smem, smem, smem, pl.BlockSpec(memory_space=pltpu.VMEM), pl.BlockSpec(memory_space=pl.ANY)],
        out_specs=pl.BlockSpec(memory_space=pltpu.VMEM),
        scratch_shapes=[
            pltpu.VMEM((cols, depth), bf16),
            pltpu.VMEM((slots, depth, blk), bf16),
            pltpu.VMEM((pieces, n, slots, width, rows), bf16),
            pltpu.VMEM((pieces, n, slots, width, rows), bf16),
            pltpu.VMEM((pieces, n, slots, width, rows), bf16),
            pltpu.VMEM((slots, width, rows), bf16),
            pltpu.VMEM((pieces, n_dom, CAP, width, rows), bf16),
            pltpu.VMEM((pieces, n_dom, CAP, width, rows), bf16),
            pltpu.VMEM((n_dom, CAP, 8, rows), f32),
            pltpu.VMEM((n_dom, CAP, 8, rows), f32),
            pltpu.VMEM((OWN, width, rows), f32),
            dma((slots,)),
            dma((pieces, n)),
            dma((pieces, n)),
            dma((pieces, n)),
            dma((pieces, n)),
            dma((pieces, n_dom)),
            dma((pieces, n_dom)),
            dma((n_dom,)),
            dma((n_dom,)),
        ],
        compiler_params=pltpu.CompilerParams(
            collective_id=0, has_side_effects=True, vmem_limit_bytes=62 * 1024 * 1024
        ),
    )(block_mask.reshape(slots), owner.reshape(slots), local_id.reshape(slots), solved[0], e_blocks[0])


def solution(mesh):
    in_specs = (
        P("dom", "grp", None),
        P("dom", None, "grp", None),
        P("dom", None, "grp"),
        P("dom", None, None),
        P("dom", None),
    )
    out_specs = P("dom", "grp", None)
    return jax.shard_map(
        on_device, mesh=mesh, in_specs=in_specs, out_specs=out_specs, check_vma=False
    )
```

```python
import functools

import jax
import jax.numpy as jnp
from jax import lax
from jax.experimental import pallas as pl
from jax.experimental.pallas import tpu as pltpu
from jax.sharding import PartitionSpec as P

OWN = 4
CAP = 2
LANES = 128
SPLIT = 2
AHEAD = 3


def kernel(
    n, n_dom, mask_ref, owner_ref, local_ref, solved_ref, e_ref, out_ref,
    factor_t, coupling, own, from_left, from_right, fin, outbox, inbox, label_out, label_in, total,
    e_sem, right_send, right_recv, left_send, left_recv, dom_send, dom_recv, label_send, label_recv,
):
    g = lax.axis_index("grp")
    me = lax.axis_index("dom")
    pieces, _, slots, width, rows = own.shape
    cols = factor_t.shape[0]

    fetches = [pltpu.make_async_copy(e_ref.at[s], coupling.at[s], e_sem.at[s]) for s in range(slots)]
    for fetch in fetches:
        fetch.start()

    barrier = pltpu.get_barrier_semaphore()

    @pl.when(g > 0)
    def _():
        pl.semaphore_signal(barrier, inc=1, device_id={"grp": g - 1})

    @pl.when(g < n - 1)
    def _():
        pl.semaphore_signal(barrier, inc=1, device_id={"grp": g + 1})

    def greet(off, carry):
        pl.semaphore_signal(barrier, inc=1, device_id={"dom": lax.rem(me + off, n_dom)})
        return carry

    lax.fori_loop(1, n_dom, greet, 0)

    for p in range(cols // LANES):
        factor_t[p * LANES:(p + 1) * LANES, :] = solved_ref[:, p * LANES:(p + 1) * LANES].T

    def multiply(low, high, fetched):
        def one(s, carry):
            if not fetched:
                pltpu.make_async_copy(e_ref.at[s], coupling.at[s], e_sem.at[s]).wait()
            present = mask_ref[s].astype(jnp.float32)
            for ch in range(n):
                product = jnp.dot(
                    factor_t[low * width:high * width, :],
                    coupling[s, :, ch * rows:(ch + 1) * rows],
                    preferred_element_type=jnp.float32,
                )
                own[low:high, ch, s] = (product * present).astype(jnp.bfloat16).reshape(high - low, width, rows)
            return carry

        lax.fori_loop(0, slots, one, 0)

    multiply(0, SPLIT, False)

    def place(d, j):
        index, label = jnp.int32(0), jnp.int32(0)
        for s in range(slots):
            position = jnp.int32(0)
            for t in range(s):
                position = position + jnp.where(owner_ref[t] == owner_ref[s], 1, 0)
            hit = jnp.where((owner_ref[s] == d) & (position == j), 1, 0)
            index = index + hit * s
            label = label + hit * (local_ref[s] + 1)
        return index, label

    def label_copy(d, source):
        return pltpu.make_async_remote_copy(
            src_ref=label_out.at[d], dst_ref=label_in.at[source],
            send_sem=label_send.at[d], recv_sem=label_recv.at[source], device_id={"dom": d},
        )

    def dom_copy(p, d, source):
        return pltpu.make_async_remote_copy(
            src_ref=outbox.at[p, d], dst_ref=inbox.at[p, source],
            send_sem=dom_send.at[p, d], recv_sem=dom_recv.at[p, source], device_id={"dom": d},
        )

    def right_copy(p, ch, source):
        return pltpu.make_async_remote_copy(
            src_ref=source.at[p, ch], dst_ref=from_left.at[p, ch],
            send_sem=right_send.at[p, ch], recv_sem=right_recv.at[p, ch], device_id={"grp": g + 1},
        )

    def left_copy(p, ch, source):
        return pltpu.make_async_remote_copy(
            src_ref=source.at[p, ch], dst_ref=from_right.at[p, ch],
            send_sem=left_send.at[p, ch], recv_sem=left_recv.at[p, ch], device_id={"grp": g - 1},
        )

    greeted = n_dom - 1 + jnp.where(g > 0, 1, 0) + jnp.where(g < n - 1, 1, 0)
    pl.semaphore_wait(barrier, greeted)

    def send_labels(off, carry):
        d = lax.rem(me + off, n_dom)
        for j in range(CAP):
            _, label = place(d, j)
            label_out[d, j] = jnp.full(label_out.shape[2:], label.astype(jnp.float32), jnp.float32)
        label_copy(d, me).start()
        return carry

    def add_to(buffer, p, ch):
        def one(s, carry):
            buffer[p, ch, s] = (
                buffer[p, ch, s].astype(jnp.float32) + own[p, ch, s].astype(jnp.float32)
            ).astype(jnp.bfloat16)
            return carry

        lax.fori_loop(0, slots, one, 0)

    def start_ends(p):
        def one(i, carry):
            to_right = n - 1 - i

            @pl.when((to_right > g) & (g == 0))
            def _():
                right_copy(p, to_right, own).start()

            @pl.when((i < g) & (g == n - 1))
            def _():
                left_copy(p, i, own).start()

            return carry

        lax.fori_loop(0, n - 1, one, 0)

    def forward(p):
        def one(i, carry):
            to_right = n - 1 - i

            @pl.when((to_right > g) & (g > 0))
            def _():
                right_copy(p, to_right, from_left).wait_recv()
                add_to(from_left, p, to_right)
                right_copy(p, to_right, from_left).start()

            @pl.when((i < g) & (g < n - 1))
            def _():
                left_copy(p, i, from_right).wait_recv()
                add_to(from_right, p, i)
                left_copy(p, i, from_right).start()

            return carry

        lax.fori_loop(0, n - 1, one, 0)

    def finish(p):
        @pl.when(g > 0)
        def _():
            right_copy(p, g, from_left).wait_recv()
            add_to(from_left, p, g)

        @pl.when(g == 0)
        def _():
            left_copy(p, g, from_right).wait_recv()
            add_to(from_right, p, g)

            def one(s, carry):
                fin[s] = from_right[p, g, s]
                return carry

            lax.fori_loop(0, slots, one, 0)

        @pl.when(g == n - 1)
        def _():
            def one(s, carry):
                fin[s] = from_left[p, g, s]
                return carry

            lax.fori_loop(0, slots, one, 0)

        @pl.when((g > 0) & (g < n - 1))
        def _():
            left_copy(p, g, from_right).wait_recv()

            def one(s, carry):
                fin[s] = (
                    from_left[p, g, s].astype(jnp.float32) + from_right[p, g, s].astype(jnp.float32)
                ).astype(jnp.bfloat16)
                return carry

            lax.fori_loop(0, slots, one, 0)

        def one_domain(off, carry):
            d = lax.rem(me + off, n_dom)
            for j in range(CAP):
                index, _ = place(d, j)
                outbox[p, d, j] = fin[index]
            dom_copy(p, d, me).start()
            return carry

        lax.fori_loop(1, n_dom, one_domain, 0)
        for j in range(CAP):
            index, _ = place(me, j)
            inbox[p, me, j] = fin[index]

    tile = 32

    def merge(p):
        def arrive(off, carry):
            source = lax.rem(me + off, n_dom)
            dom_copy(p, source, source).wait_recv()
            return carry

        lax.fori_loop(1, n_dom, arrive, 0)

        half = lax.rem(p, SPLIT) * width

        def one(t, carry):
            at = pl.ds(pl.multiple_of(t * tile, tile), tile)
            put = pl.ds(pl.multiple_of(half + t * tile, tile), tile)
            sums = [jnp.zeros((tile, rows), jnp.float32) for _ in range(OWN)]
            for source in range(n_dom):
                for j in range(CAP):
                    block = inbox[p, source, j, at, :].astype(jnp.float32)
                    label = label_in[source, j, 0:1, :]
                    for o in range(OWN):
                        sums[o] = sums[o] + block * jnp.where(label == o + 1, 1.0, 0.0)
            for o in range(OWN):
                total[o, put, :] = sums[o]
            return carry

        lax.fori_loop(0, width // tile, one, 0)
        @pl.when(lax.rem(p, SPLIT) == SPLIT - 1)
        def _():
            lanes = pl.ds(pl.multiple_of((p // SPLIT) * LANES, LANES), LANES)
            for o in range(OWN):
                out_ref[o, :, lanes] = total[o].T.astype(jnp.bfloat16)

    for p in range(SPLIT):
        start_ends(p)
    multiply(SPLIT, pieces, True)
    for p in range(SPLIT, AHEAD):
        start_ends(p)
    lax.fori_loop(1, n_dom, send_labels, 0)
    for j in range(CAP):
        _, label = place(me, j)
        label_in[me, j] = jnp.full(label_out.shape[2:], label.astype(jnp.float32), jnp.float32)
    def step(p, carry):
        @pl.when(p + AHEAD < pieces)
        def _():
            start_ends(p + AHEAD)

        forward(p)
        finish(p)

        @pl.when(p == 0)
        def _():
            def labelled(off, carry):
                source = lax.rem(me + off, n_dom)
                label_copy(source, source).wait_recv()
                return carry

            lax.fori_loop(1, n_dom, labelled, 0)

        @pl.when(p > 0)
        def _():
            merge(p - 1)

        return carry

    lax.fori_loop(0, pieces, step, 0)
    merge(jnp.int32(pieces - 1))

    def drain_dom(off, carry):
        d = lax.rem(me + off, n_dom)
        label_copy(d, me).wait_send()
        for p in range(pieces):
            dom_copy(p, d, me).wait_send()
        return carry

    lax.fori_loop(1, n_dom, drain_dom, 0)

    def drain(ch, carry):
        for p in range(pieces):
            @pl.when(ch > g)
            def _():
                right_copy(p, ch, from_left).wait_send()

            @pl.when(ch < g)
            def _():
                left_copy(p, ch, from_right).wait_send()

        return carry

    lax.fori_loop(0, n, drain, 0)


def on_device(solved, e_blocks, block_mask, owner, local_id):
    n, n_dom = lax.axis_size("grp"), lax.axis_size("dom")
    _, depth, cols = solved.shape
    slots, blk = e_blocks.shape[1], e_blocks.shape[3]
    rows, width = blk // n, LANES // SPLIT
    pieces = cols // width
    bf16, f32 = jnp.bfloat16, jnp.float32
    smem = pl.BlockSpec(memory_space=pltpu.SMEM)
    dma = pltpu.SemaphoreType.DMA
    return pl.pallas_call(
        functools.partial(kernel, n, n_dom),
        out_shape=jax.ShapeDtypeStruct((OWN, rows, cols), bf16),
        in_specs=[smem, smem, smem, pl.BlockSpec(memory_space=pltpu.VMEM), pl.BlockSpec(memory_space=pl.ANY)],
        out_specs=pl.BlockSpec(memory_space=pltpu.VMEM),
        scratch_shapes=[
            pltpu.VMEM((cols, depth), bf16),
            pltpu.VMEM((slots, depth, blk), bf16),
            pltpu.VMEM((pieces, n, slots, width, rows), bf16),
            pltpu.VMEM((pieces, n, slots, width, rows), bf16),
            pltpu.VMEM((pieces, n, slots, width, rows), bf16),
            pltpu.VMEM((slots, width, rows), bf16),
            pltpu.VMEM((pieces, n_dom, CAP, width, rows), bf16),
            pltpu.VMEM((pieces, n_dom, CAP, width, rows), bf16),
            pltpu.VMEM((n_dom, CAP, 8, rows), f32),
            pltpu.VMEM((n_dom, CAP, 8, rows), f32),
            pltpu.VMEM((OWN, LANES, rows), f32),
            dma((slots,)),
            dma((pieces, n)),
            dma((pieces, n)),
            dma((pieces, n)),
            dma((pieces, n)),
            dma((pieces, n_dom)),
            dma((pieces, n_dom)),
            dma((n_dom,)),
            dma((n_dom,)),
        ],
        compiler_params=pltpu.CompilerParams(
            collective_id=0, has_side_effects=True, vmem_limit_bytes=62 * 1024 * 1024
        ),
    )(block_mask.reshape(slots), owner.reshape(slots), local_id.reshape(slots), solved[0], e_blocks[0])


def solution(mesh):
    in_specs = (
        P("dom", "grp", None),
        P("dom", None, "grp", None),
        P("dom", None, "grp"),
        P("dom", None, None),
        P("dom", None),
    )
    out_specs = P("dom", "grp", None)
    return jax.shard_map(
        on_device, mesh=mesh, in_specs=in_specs, out_specs=out_specs, check_vma=False
    )
```
